16 devices in a mesh: dp: 4 (over z, y), cp: 4 (over x, core).
Axes of the slice: x: 2, y: 2, z: 2, core: 2. Of those that a mesh axis runs over, the one named last changes fastest.
Arguments:
- x_in: bfloat16 [4, 2048, 1536], P('dp', 'cp')
- d_out: bfloat16 [4, 2048, 1536], P('dp', 'cp')
- w_q: bfloat16 [1536, 12, 128], replicated
- w_k: bfloat16 [1536, 2, 128], replicated
- w_v: bfloat16 [1536, 2, 128], replicated
- w_o: bfloat16 [12, 128, 1536], replicated
- w_up: bfloat16 [1536, 8960], replicated
- w_down: bfloat16 [8960, 1536], replicated
Outputs:
- output 1: bfloat16 [4, 2048, 1536], P('dp', 'cp')
- output 2: float32 [1536, 12, 128], replicated
- output 3: float32 [1536, 2, 128], replicated
- output 4: float32 [1536, 2, 128], replicated
- output 5: float32 [12, 128, 1536], replicated
- output 6: float32 [1536, 8960], replicated
- output 7: float32 [8960, 1536], replicated
All inputs are finite; a program needn't handle non-finite values.
Results may differ from the reference program's by a relative error of at most 0.02.
Values are sent between devices in bfloat16 or wider.
A program may use at most 1 GiB of HBM per device.

```python
import jax
import jax.numpy as jnp
from jax import lax

MODEL_WIDTH = 1536
NUM_HEADS = 12
KV_HEADS = 2
HEAD_DIM = 128
FFN_WIDTH = 8960
BATCH_SIZE = 4
SEQ_LEN = 2048
QUERY_BLOCK = 512
GRAD_DIVISOR = 16

GROUP_SIZE = NUM_HEADS // KV_HEADS
SCORE_SCALE = HEAD_DIM ** -0.5


def setup_inputs(seed: int = 0) -> dict:
    rng_keys = jax.random.split(jax.random.key(seed), 8)
    act_shape = (BATCH_SIZE, SEQ_LEN, MODEL_WIDTH)

    def draw_weight(one_key, shape, fan_in, weight_gain):
        values = jax.random.normal(one_key, shape, jnp.float32) * (weight_gain * fan_in ** -0.5)
        return values.astype(jnp.bfloat16)

    return {
        'x_in': jax.random.normal(rng_keys[0], act_shape, jnp.float32).astype(jnp.bfloat16),
        'd_out': jax.random.normal(rng_keys[1], act_shape, jnp.float32).astype(jnp.bfloat16),
        'w_q': draw_weight(rng_keys[2], (MODEL_WIDTH, NUM_HEADS, HEAD_DIM), MODEL_WIDTH, 2.5),
        'w_k': draw_weight(rng_keys[3], (MODEL_WIDTH, KV_HEADS, HEAD_DIM), MODEL_WIDTH, 1.0),
        'w_v': draw_weight(rng_keys[4], (MODEL_WIDTH, KV_HEADS, HEAD_DIM), MODEL_WIDTH, 1.0),
        'w_o': draw_weight(rng_keys[5], (NUM_HEADS, HEAD_DIM, MODEL_WIDTH), NUM_HEADS * HEAD_DIM, 1.5),
        'w_up': draw_weight(rng_keys[6], (MODEL_WIDTH, FFN_WIDTH), MODEL_WIDTH, 1.0),
        'w_down': draw_weight(rng_keys[7], (FFN_WIDTH, MODEL_WIDTH), FFN_WIDTH, 1.0),
    }


def block_attention(q_block, k_seq, v_seq):
    scores = jnp.einsum('qkgd,pkd->kgqp', q_block, k_seq) * SCORE_SCALE
    prob_rounded = jax.nn.softmax(scores, axis=-1).astype(jnp.bfloat16).astype(jnp.float32)
    return jnp.einsum('kgqp,pkd->qkgd', prob_rounded, v_seq)


checked_attention = jax.checkpoint(block_attention)


def attend_sequence(operands):
    q_seq, k_seq, v_seq = operands
    q_blocks = q_seq.reshape(SEQ_LEN // QUERY_BLOCK, QUERY_BLOCK, KV_HEADS, GROUP_SIZE, HEAD_DIM)
    out_blocks = lax.map(lambda q_block: checked_attention(q_block, k_seq, v_seq), q_blocks)
    return out_blocks.reshape(SEQ_LEN, KV_HEADS, GROUP_SIZE, HEAD_DIM)


def layer_forward(x_in, w_q, w_k, w_v, w_o, w_up, w_down):
    row_count = BATCH_SIZE * SEQ_LEN
    x_rows = x_in.reshape(row_count, MODEL_WIDTH).astype(jnp.float32)

    def project(weight, head_count):
        product = jnp.dot(x_rows, weight.reshape(MODEL_WIDTH, head_count * HEAD_DIM), preferred_element_type=jnp.float32)
        return product.astype(jnp.bfloat16).astype(jnp.float32)

    q_all = project(w_q, NUM_HEADS).reshape(BATCH_SIZE, SEQ_LEN, KV_HEADS, GROUP_SIZE, HEAD_DIM)
    k_all = project(w_k, KV_HEADS).reshape(BATCH_SIZE, SEQ_LEN, KV_HEADS, HEAD_DIM)
    v_all = project(w_v, KV_HEADS).reshape(BATCH_SIZE, SEQ_LEN, KV_HEADS, HEAD_DIM)
    attn_out = lax.map(attend_sequence, (q_all, k_all, v_all))
    attn_rows = attn_out.astype(jnp.bfloat16).astype(jnp.float32).reshape(row_count, NUM_HEADS * HEAD_DIM)
    out_proj = jnp.dot(attn_rows, w_o.reshape(NUM_HEADS * HEAD_DIM, MODEL_WIDTH), preferred_element_type=jnp.float32)
    hidden = (x_rows + out_proj).astype(jnp.bfloat16).astype(jnp.float32)
    up_proj = jnp.dot(hidden, w_up, preferred_element_type=jnp.float32)
    gated = jax.nn.gelu(up_proj, approximate=True).astype(jnp.bfloat16).astype(jnp.float32)
    out_rows = hidden + jnp.dot(gated, w_down, preferred_element_type=jnp.float32)
    return out_rows.astype(jnp.bfloat16).reshape(BATCH_SIZE, SEQ_LEN, MODEL_WIDTH)


def reference(x_in, d_out, w_q, w_k, w_v, w_o, w_up, w_down):
    layer_vjp = jax.vjp(layer_forward, x_in, w_q.astype(jnp.float32), w_k.astype(jnp.float32), w_v.astype(jnp.float32), w_o.astype(jnp.float32), w_up.astype(jnp.float32), w_down.astype(jnp.float32))[1]
    cotangents = layer_vjp(d_out)
    return (cotangents[0], cotangents[1] / GRAD_DIVISOR, cotangents[2] / GRAD_DIVISOR, cotangents[3] / GRAD_DIVISOR, cotangents[4] / GRAD_DIVISOR, cotangents[5] / GRAD_DIVISOR, cotangents[6] / GRAD_DIVISOR)
```

```python
import functools
import jax
import jax.numpy as jnp
from jax import lax
from jax.experimental import pallas as pl
from jax.experimental.pallas import tpu as pltpu
from jax.sharding import PartitionSpec as P

f32, bf16 = jnp.float32, jnp.bfloat16
NN = (((1,), (0,)), ((), ()))
NT = (((1,), (1,)), ((), ()))
TN = (((0,), (0,)), ((), ()))
TT = (((0,), (1,)), ((), ()))
LOG2E = 1.4426950408889634
GELU_A = 0.7978845608028654
GELU_B = GELU_A * 0.044715
MIB = 1 << 20
LANES = 128
UNIT_ROWS = 32


def dot(a, b, dims):
    return lax.dot_general(a, b, dims, preferred_element_type=f32)


def params(rank, vmem):
    return pltpu.CompilerParams(dimension_semantics=('arbitrary',) * rank, vmem_limit_bytes=vmem * MIB)


def attn_fwd_kernel(heads_step, coef, head_dim, q_ref, k_ref, v_ref, a_ref, l_ref):
    for i in range(heads_step):
        cols = slice(i * head_dim, (i + 1) * head_dim)
        scores = dot(k_ref[:], q_ref[:, cols], NT)
        top = jnp.max(scores, axis=0, keepdims=True)
        probs = jnp.exp2((scores - top) * coef)
        total = jnp.sum(probs, axis=0, keepdims=True)
        out_t = dot(v_ref[:], probs.astype(bf16), TN)
        a_ref[:, cols] = (out_t * (1.0 / total)).T.astype(bf16)
        l_ref[i] = jnp.broadcast_to(top * coef + jnp.log2(total), l_ref.shape[1:])


def attn_fwd(q, kv, heads, kv_heads, head_dim, coef):
    rows, keys = q.shape[0], kv.shape[0]
    step = heads // kv_heads // 2
    per = heads // kv_heads // step
    q_spec = pl.BlockSpec((rows, step * head_dim), lambda h: (0, h))
    return pl.pallas_call(
        functools.partial(attn_fwd_kernel, step, coef, head_dim),
        grid=(heads // step,),
        in_specs=[q_spec, pl.BlockSpec((keys, head_dim), lambda h: (0, h // per)), pl.BlockSpec((keys, head_dim), lambda h: (0, kv_heads + h // per))],
        out_specs=[q_spec, pl.BlockSpec((step, 8, rows), lambda h: (h, 0, 0))],
        out_shape=[jax.ShapeDtypeStruct(q.shape, bf16), jax.ShapeDtypeStruct((heads, 8, rows), f32)],
        compiler_params=params(1, 60),
        cost_estimate=pl.CostEstimate(flops=8 * rows * keys * head_dim * heads, bytes_accessed=8 * MIB, transcendentals=rows * keys * heads),
        name='attn_fwd',
    )(q, kv, kv)


def attn_bwd_kernel(heads_step, steps, coef, scale, head_dim, q_ref, k_ref, v_ref, a_ref, da_ref, l_ref, dq_ref, dk_ref, dv_ref):
    @pl.when(pl.program_id(1) == 0)
    def _():
        dk_ref[:] = jnp.zeros_like(dk_ref)
        dv_ref[:] = jnp.zeros_like(dv_ref)

    for i in range(heads_step):
        cols = slice(i * head_dim, (i + 1) * head_dim)
        q, da = q_ref[:, cols], da_ref[:, cols]
        delta = jnp.sum((da.astype(f32) * a_ref[:, cols].astype(f32)).T, axis=0, keepdims=True)
        probs = jnp.exp2(dot(k_ref[:], q, NT) * coef - l_ref[i, 0:1, :])
        d_probs = dot(v_ref[:], da, NT)
        d_scores = (probs * (d_probs - delta)).astype(bf16)
        dv_ref[:] += dot(probs.astype(bf16), da, NN)
        dk_ref[:] += dot(d_scores, q, NN)
        dq_ref[:, cols] = (dot(k_ref[:], d_scores, TN) * scale).T.astype(bf16)

    @pl.when(pl.program_id(1) == steps - 1)
    def _():
        dk_ref[:] = dk_ref[:] * scale


def attn_bwd(q, kv, a, da, lse, heads, kv_heads, head_dim, coef, scale):
    rows, keys = q.shape[0], kv.shape[0]
    step = heads // kv_heads // 2
    steps = heads // kv_heads // step
    q_spec = pl.BlockSpec((rows, step * head_dim), lambda g, h: (0, g * steps + h))
    kv_spec = pl.BlockSpec((keys, head_dim), lambda g, h: (0, g))
    kv_shape = jax.ShapeDtypeStruct((keys, kv_heads * head_dim), f32)
    return pl.pallas_call(
        functools.partial(attn_bwd_kernel, step, steps, coef, scale, head_dim),
        grid=(kv_heads, steps),
        in_specs=[q_spec, kv_spec, pl.BlockSpec((keys, head_dim), lambda g, h: (0, kv_heads + g)), q_spec, q_spec, pl.BlockSpec((step, 8, rows), lambda g, h: (g * steps + h, 0, 0))],
        out_specs=[q_spec, kv_spec, kv_spec],
        out_shape=[jax.ShapeDtypeStruct(q.shape, bf16), kv_shape, kv_shape],
        compiler_params=params(2, 62),
        cost_estimate=pl.CostEstimate(flops=14 * rows * keys * head_dim * heads, bytes_accessed=16 * MIB, transcendentals=rows * keys * heads),
        name='attn_bwd',
    )(q, kv, kv, a, da, lse)


def gelu_pair(u, d_gated):
    square = u * u
    a = 0.5 * jnp.tanh(u * (GELU_A + GELU_B * square)) + 0.5
    gated = u * a
    slope = a + (gated - gated * a) * (2 * GELU_A + (6 * GELU_B) * square)
    return gated, slope * d_gated


def q_proj_kernel(x_ref, w_ref, o_ref):
    pair = jnp.concatenate([w_ref[0], w_ref[1]], axis=1)
    o_ref[:] = dot(x_ref[:], pair, NN).astype(bf16)


def q_proj(x, w_heads):
    rows, depth = x.shape
    heads, _, head_dim = w_heads.shape
    return pl.pallas_call(
        q_proj_kernel,
        grid=(heads // 2,),
        in_specs=[pl.BlockSpec((rows, depth), lambda i: (0, 0)), pl.BlockSpec((2, depth, head_dim), lambda i: (i, 0, 0))],
        out_specs=pl.BlockSpec((rows, 2 * head_dim), lambda i: (0, i)),
        out_shape=jax.ShapeDtypeStruct((rows, heads * head_dim), bf16),
        compiler_params=params(1, 60),
        cost_estimate=pl.CostEstimate(flops=2 * rows * depth * heads * head_dim, bytes_accessed=8 * MIB, transcendentals=0),
        name='q_proj',
    )(x, w_heads)


def d_input_kernel(steps, dh_ref, dkv_ref, wkv_ref, dq_ref, w_ref, o_ref, acc):
    i = pl.program_id(0)

    @pl.when(i == 0)
    def _():
        acc[:] = dh_ref[:].astype(f32) + dot(dkv_ref[:], wkv_ref[:], NT)

    pair = jnp.concatenate([w_ref[0], w_ref[1]], axis=1)
    acc[:] += dot(dq_ref[:], pair, NT)

    @pl.when(i == steps - 1)
    def _():
        o_ref[:] = acc[:].astype(bf16)


def d_input(d_hidden, d_kv, w_kv, d_q, w_heads):
    rows, depth = d_hidden.shape
    heads, _, head_dim = w_heads.shape
    whole = lambda array: pl.BlockSpec(array.shape, lambda i: (0, 0))
    return pl.pallas_call(
        functools.partial(d_input_kernel, heads // 2),
        grid=(heads // 2,),
        in_specs=[whole(d_hidden), whole(d_kv), whole(w_kv), pl.BlockSpec((rows, 2 * head_dim), lambda i: (0, i)), pl.BlockSpec((2, depth, head_dim), lambda i: (i, 0, 0))],
        out_specs=whole(d_hidden),
        out_shape=jax.ShapeDtypeStruct((rows, depth), bf16),
        scratch_shapes=[pltpu.VMEM((rows, depth), f32)],
        compiler_params=params(1, 60),
        cost_estimate=pl.CostEstimate(flops=2 * rows * depth * heads * head_dim, bytes_accessed=12 * MIB, transcendentals=0),
        name='d_input',
    )(d_hidden, d_kv, w_kv, d_q, w_heads)


def own_gate_kernel(do_ref, wd_ref, o_ref):
    o_ref[:] = dot(do_ref[:], wd_ref[:], NT).astype(bf16)


def own_gate(d_out, w_down, block):
    rows, depth = d_out.shape
    width = w_down.shape[0]
    return pl.pallas_call(
        own_gate_kernel,
        grid=(width // block,),
        in_specs=[pl.BlockSpec((rows, depth), lambda i: (0, 0)), pl.BlockSpec((block, depth), lambda i: (i, 0))],
        out_specs=pl.BlockSpec((rows, block), lambda i: (0, i)),
        out_shape=jax.ShapeDtypeStruct((rows, width), bf16),
        compiler_params=params(1, 60),
        cost_estimate=pl.CostEstimate(flops=2 * rows * width * depth, bytes_accessed=2 * width * (depth + rows), transcendentals=0),
        name='own_gate',
    )(d_out, w_down)


def own_mlp_kernel(steps, parts, h_ref, do_ref, dg_ref, wu_ref, o_ref, acc):
    i = pl.program_id(0)

    @pl.when(i == 0)
    def _():
        acc[:] = do_ref[:].astype(f32)

    width = wu_ref.shape[1] // parts
    d_up = []
    for j in range(parts):
        cols = slice(j * width, (j + 1) * width)
        up = dot(h_ref[:], wu_ref[:, cols], NN)
        d_up.append(gelu_pair(up, dg_ref[:, cols].astype(f32))[1].astype(bf16))
    acc[:] += dot(jnp.concatenate(d_up, axis=1), wu_ref[:], NT)

    @pl.when(i == steps - 1)
    def _():
        o_ref[:] = acc[:].astype(bf16)


def own_mlp(hidden, d_out, dg, w_up, block, parts):
    rows, depth = hidden.shape
    width = w_up.shape[1]
    full = pl.BlockSpec((rows, depth), lambda i: (0, 0))
    return pl.pallas_call(
        functools.partial(own_mlp_kernel, width // block, parts),
        grid=(width // block,),
        in_specs=[full, full, pl.BlockSpec((rows, block), lambda i: (0, i)), pl.BlockSpec((depth, block), lambda i: (0, i))],
        out_specs=full,
        out_shape=jax.ShapeDtypeStruct((rows, depth), bf16),
        scratch_shapes=[pltpu.VMEM((rows, depth), f32)],
        compiler_params=params(1, 60),
        cost_estimate=pl.CostEstimate(flops=4 * rows * width * depth, bytes_accessed=2 * width * (depth + rows), transcendentals=rows * width),
        name='own_mlp',
    )(hidden, d_out, dg, w_up)


def attn_wgrad_kernel(kv_end, scale, ids, x_ref, a_ref, rhs_ref, keep_ref, give_ref, xt, at):
    i = pl.program_id(0)

    @pl.when(i == 0)
    def _():
        xt[:] = x_ref[:].T
        at[:] = a_ref[:].T

    half = xt.shape[0] // 2

    def emit(lhs):
        for side, target in ((ids[0], keep_ref), (1 - ids[0], give_ref)):
            product = dot(lhs[pl.ds(pl.multiple_of(side * half, UNIT_ROWS), half), :], rhs_ref[:], NN) * scale
            for j in range(target.shape[1]):
                target[:, j] = product[:, j * LANES:(j + 1) * LANES].reshape(target.shape[0], UNIT_ROWS, LANES)

    @pl.when(i < kv_end)
    def _():
        emit(xt)

    @pl.when(i >= kv_end)
    def _():
        emit(at)


def attn_wgrad(core, x, a, rhs, kv_end, scale):
    rows, depth = x.shape
    width = rhs.shape[1]
    units = depth // UNIT_ROWS // 2
    full = pl.BlockSpec((rows, depth), lambda i, ids: (0, 0))
    out_spec = pl.BlockSpec((units, 2, UNIT_ROWS, LANES), lambda i, ids: (0, i, 0, 0))
    return pl.pallas_call(
        functools.partial(attn_wgrad_kernel, kv_end, scale),
        grid_spec=pltpu.PrefetchScalarGridSpec(
            num_scalar_prefetch=1,
            grid=(width // (2 * LANES),),
            in_specs=[full, full, pl.BlockSpec((rows, 2 * LANES), lambda i, ids: (0, i))],
            out_specs=[out_spec, out_spec],
            scratch_shapes=[pltpu.VMEM((depth, rows), bf16), pltpu.VMEM((depth, rows), bf16)],
        ),
        out_shape=[jax.ShapeDtypeStruct((units, width // LANES, UNIT_ROWS, LANES), f32)] * 2,
        compiler_params=params(1, 60),
        cost_estimate=pl.CostEstimate(flops=2 * rows * width * depth, bytes_accessed=4 * width * depth, transcendentals=0),
        name='attn_wgrad',
    )(core, x, a, rhs)


def attn_unpack_kernel(unit_of, splits, in_ref, q_ref, k_ref, v_ref, o_ref):
    i = pl.program_id(0)
    first, second = splits

    def each(store):
        for device, colour, unit in unit_of:
            for j in range(2):
                store(slice(unit * UNIT_ROWS, (unit + 1) * UNIT_ROWS), j, in_ref[device, colour, j])

    @pl.when(i < first)
    def _():
        def store(rows, j, value):
            q_ref[j, rows] = value

        each(store)

    for n, target in enumerate((k_ref, v_ref)):
        @pl.when(i == first + n)
        def _(target=target):
            def store(rows, j, value):
                target[rows, j] = value

            each(store)

    @pl.when(i >= second)
    def _():
        def store(rows, j, value):
            o_ref[rows, j * LANES:(j + 1) * LANES] = value

        each(store)


def attn_unpack(gathered, unit_of, splits, depth):
    devices, colours, slabs = gathered.shape[:3]
    first, second = splits
    kv_spec = pl.BlockSpec((depth, 2, LANES), lambda i: (0, 0, 0), pipeline_mode=pl.Buffered(1))
    kv_shape = jax.ShapeDtypeStruct((depth, 2, LANES), f32)
    return pl.pallas_call(
        functools.partial(attn_unpack_kernel, unit_of, splits),
        grid=(slabs // 2,),
        in_specs=[pl.BlockSpec((devices, colours, 2, UNIT_ROWS, LANES), lambda i: (0, 0, i, 0, 0))],
        out_specs=[
            pl.BlockSpec((2, depth, LANES), lambda i: (jnp.minimum(i, first - 1), 0, 0)),
            kv_spec,
            kv_spec,
            pl.BlockSpec((depth, 2 * LANES), lambda i: (0, jnp.maximum(i - second, 0))),
        ],
        out_shape=[jax.ShapeDtypeStruct((2 * first, depth, LANES), f32), kv_shape, kv_shape, jax.ShapeDtypeStruct((depth, (slabs - 2 * second) * LANES), f32)],
        compiler_params=params(1, 60),
        cost_estimate=pl.CostEstimate(flops=0, bytes_accessed=2 * gathered.size * 4, transcendentals=0),
        name='attn_unpack',
    )(gathered)


def d_gate_kernel(ids, w_ref, do_ref, o_ref):
    o_ref[:] = dot(w_ref[:], do_ref[:], NT).astype(bf16)


def d_gate(base, w_down, d_out, width, block, tile):
    depth = w_down.shape[1]
    rows = d_out.shape[0]
    return pl.pallas_call(
        d_gate_kernel,
        grid_spec=pltpu.PrefetchScalarGridSpec(
            num_scalar_prefetch=1,
            grid=(width // block, rows // tile),
            in_specs=[pl.BlockSpec((block, depth), lambda i, t, ids: (ids[0] + i, 0)), pl.BlockSpec((tile, depth), lambda i, t, ids: (t, 0))],
            out_specs=pl.BlockSpec((block, tile), lambda i, t, ids: (i, t)),
        ),
        out_shape=jax.ShapeDtypeStruct((width, rows), bf16),
        compiler_params=params(2, 60),
        cost_estimate=pl.CostEstimate(flops=2 * width * depth * rows, bytes_accessed=2 * (width * depth + rows * depth + width * rows), transcendentals=0),
        name='d_gate',
    )(base, w_down, d_out)


def mesh_bits():
    dp, cp = lax.axis_index('dp'), lax.axis_index('cp')
    return dp, cp, {'z': dp // 2, 'y': lax.rem(dp, 2), 'x': cp // 2, 'core': lax.rem(cp, 2)}


def neighbour(dp, cp, bits, axis):
    flip = 1 - 2 * bits[axis]
    return {'x': (dp, cp + 2 * flip), 'y': (dp + flip, cp), 'z': (dp + 2 * flip, cp)}[axis]


def rs_bit(bits, colour_axes, colour, level):
    return bits[colour_axes[colour][level]]


def greet(axes, dp, cp, bits):
    barrier = pltpu.get_barrier_semaphore()
    for axis in axes:
        pl.semaphore_signal(barrier, inc=1, device_id=neighbour(dp, cp, bits, axis), device_id_type=pl.DeviceIdType.MESH)
    pl.semaphore_wait(barrier, len(axes))


def shared_grad_kernel(steps, chunk, scale, colour_axes, w_ref, dg_ref, h_ref, do_ref, keep_ref, recv_ref, out_ref, mine, w_t, g_s, d_s, acc_up, acc_down, send, other, incoming, load_sem, send_sem, recv_sem):
    t = pl.program_id(0)
    block, tile = g_s.shape
    dp, cp, bits = mesh_bits()
    colours = range(len(colour_axes))

    def load(kind, colour):
        first = rs_bit(bits, colour_axes, colour, 0)
        side = first if kind % 2 else 1 - first
        units = pl.ds(8 * colour + 4 * side, 4)
        source = (keep_ref, recv_ref)[kind // 2].at[units]
        target = (send, mine, other, other)[kind].at[colour]
        return pltpu.make_async_copy(source, target, load_sem.at[kind, colour])

    def exchange(colour):
        target = neighbour(dp, cp, bits, colour_axes[colour][0])
        return pltpu.make_async_remote_copy(src_ref=send.at[colour], dst_ref=incoming.at[colour], send_sem=send_sem.at[colour], recv_sem=recv_sem.at[colour], device_id=target, device_id_type=pl.DeviceIdType.MESH)

    @pl.when(t == 0)
    def _():
        for colour in colours:
            load(0, colour).start()
            load(2, colour).start()
        greet(('x', 'y', 'z'), dp, cp, bits)
        w_t[:] = w_ref[:].T
        for colour in colours:
            load(0, colour).wait()
            load(2, colour).wait()
            send[colour] = send[colour] + other[colour]
        for colour in colours:
            exchange(colour).start()
            load(1, colour).start()
            load(3, colour).start()
        acc_up[:] = jnp.zeros(acc_up.shape, f32)
        acc_down[:] = jnp.zeros(acc_down.shape, f32)

    @pl.when(t == 1)
    def _():
        for kind in (1, 3):
            for colour in colours:
                load(kind, colour).wait()
        for colour in colours:
            mine[colour] = mine[colour] + other[colour]

    for j in range(tile // chunk):
        s = pl.ds(j * chunk, chunk)
        gated, d_up = gelu_pair(dot(w_t[:], h_ref[s, :], NT), dg_ref[:, s].astype(f32))
        g_s[:, s] = gated.astype(bf16)
        d_s[:, s] = d_up.astype(bf16)
    acc_down[:] += dot(g_s[:], do_ref[:], NN)
    acc_up[:] += dot(h_ref[:], d_s[:], TT)

    @pl.when(t == steps - 1)
    def _():
        out_ref[:block] = acc_down[:] * scale
        for j in range(acc_up.shape[0] // block):
            out_ref[block:, j * block:(j + 1) * block] = acc_up[j * block:(j + 1) * block, :] * scale
        for colour in colours:
            exchange(colour).wait()
            mine[colour] = mine[colour] + incoming[colour]


def shared_grad(w_up, dg, hidden, d_out, keep, recv, shared, tile, chunk, scale, colour_axes):
    block, base = shared
    depth, rows = w_up.shape[0], hidden.shape[0]
    steps, colours = rows // tile, len(colour_axes)
    half = (colours, 4) + keep.shape[1:]
    tile_spec = pl.BlockSpec((tile, depth), lambda t: (t, 0))
    any_spec = pl.BlockSpec(memory_space=pl.ANY)
    once = pl.Buffered(1)

    def device():
        return lax.axis_index('dp') * lax.axis_size('cp') + lax.axis_index('cp')

    return pl.pallas_call(
        functools.partial(shared_grad_kernel, steps, chunk, scale, colour_axes),
        grid=(steps,),
        in_specs=[pl.BlockSpec((depth, block), lambda t: (0, base + device()), pipeline_mode=once), pl.BlockSpec((block, tile), lambda t: (0, t)), tile_spec, tile_spec, any_spec, any_spec],
        out_specs=[pl.BlockSpec((2 * block, depth), lambda t: (0, 0), pipeline_mode=once), pl.BlockSpec(half, lambda t: (0,) * len(half), pipeline_mode=once)],
        out_shape=[jax.ShapeDtypeStruct((2 * block, depth), f32), jax.ShapeDtypeStruct(half, f32)],
        scratch_shapes=[
            pltpu.VMEM((block, depth), bf16), pltpu.VMEM((block, tile), bf16), pltpu.VMEM((block, tile), bf16), pltpu.VMEM((depth, block), f32), pltpu.VMEM((block, depth), f32),
            pltpu.VMEM(half, f32), pltpu.VMEM(half, f32), pltpu.VMEM(half, f32),
            pltpu.SemaphoreType.DMA((4, colours)), pltpu.SemaphoreType.DMA((colours,)), pltpu.SemaphoreType.DMA((colours,)),
        ],
        compiler_params=pltpu.CompilerParams(dimension_semantics=('arbitrary',), vmem_limit_bytes=63 * MIB, collective_id=0, has_side_effects=True),
        cost_estimate=pl.CostEstimate(flops=6 * block * depth * rows, bytes_accessed=4 * rows * depth, transcendentals=block * rows),
        name='shared_grad',
    )(w_up, dg, hidden, d_out, keep, recv)


def gate_reduce_kernel(steps, ready, colour_axes, w_ref, do_ref, mine, gate_ref, sum_ref, rest, in2, in3, load_sem, send_sem, recv_sem):
    s = pl.program_id(0)
    dp, cp, bits = mesh_bits()
    colours = range(len(colour_axes))

    def exchange(level, colour):
        if level == 1:
            side = 1 - rs_bit(bits, colour_axes, colour, 1)
            src, dst = mine.at[colour, pl.ds(2 * side, 2)], in2.at[colour]
        else:
            src, dst = rest.at[colour, pl.ds(1 - rs_bit(bits, colour_axes, colour, 2), 1)], in3.at[colour]
        target = neighbour(dp, cp, bits, colour_axes[colour][level])
        return pltpu.make_async_remote_copy(src_ref=src, dst_ref=dst, send_sem=send_sem.at[level - 1, colour], recv_sem=recv_sem.at[level - 1, colour], device_id=target, device_id_type=pl.DeviceIdType.MESH)

    def load(colour):
        return pltpu.make_async_copy(mine.at[colour, pl.ds(2 * rs_bit(bits, colour_axes, colour, 1), 2)], rest.at[colour], load_sem.at[colour])

    @pl.when(s == 0)
    def _():
        greet(('x', 'y', 'z'), dp, cp, bits)
        for colour in colours:
            exchange(1, colour).start()
            load(colour).start()

    @pl.when(s == ready)
    def _():
        for colour in colours:
            exchange(1, colour).wait()
            load(colour).wait()
            rest[colour] = rest[colour] + in2[colour]
        for colour in colours:
            exchange(2, colour).start()

    gate_ref[:] = dot(w_ref[:], do_ref[:], NT).astype(bf16)

    @pl.when(s == steps - 1)
    def _():
        for colour in colours:
            exchange(2, colour).wait()
            sum_ref[colour] = rest[colour, rs_bit(bits, colour_axes, colour, 2)] + in3[colour, 0]


def gate_reduce(w_down, d_out, mine, gate, tile, colour_axes):
    block, count, base = gate
    depth, rows = w_down.shape[1], d_out.shape[0]
    tiles = rows // tile
    steps = count * tiles
    colours = len(colour_axes)
    slab = mine.shape[2:]
    once = pl.Buffered(1)
    return pl.pallas_call(
        functools.partial(gate_reduce_kernel, steps, 2 * steps // 3, colour_axes),
        grid=(steps,),
        in_specs=[
            pl.BlockSpec((block, depth), lambda s: (base + count * lax.rem(lax.axis_index('cp'), 2) + s // tiles, 0)),
            pl.BlockSpec((tile, depth), lambda s: (s % tiles, 0)),
            pl.BlockSpec(memory_space=pl.ANY),
        ],
        out_specs=[
            pl.BlockSpec((block, tile), lambda s: (s // tiles, s % tiles)),
            pl.BlockSpec((colours,) + slab, lambda s: (0, 0, 0, 0), pipeline_mode=once),
        ],
        out_shape=[jax.ShapeDtypeStruct((block * count, rows), bf16), jax.ShapeDtypeStruct((colours,) + slab, f32)],
        scratch_shapes=[
            pltpu.VMEM((colours, 2) + slab, f32), pltpu.VMEM((colours, 2) + slab, f32), pltpu.VMEM((colours, 1) + slab, f32),
            pltpu.SemaphoreType.DMA((colours,)), pltpu.SemaphoreType.DMA((2, colours)), pltpu.SemaphoreType.DMA((2, colours)),
        ],
        compiler_params=pltpu.CompilerParams(dimension_semantics=('arbitrary',), vmem_limit_bytes=63 * MIB, collective_id=1, has_side_effects=True),
        cost_estimate=pl.CostEstimate(flops=2 * depth * rows * block * count, bytes_accessed=100 * MIB, transcendentals=0),
        name='gate_reduce',
    )(w_down, d_out, mine)


def partner_moves(start, width, rows, partner, up_src, down_src, up_full, down_full):
    depth = up_full.shape[0]
    offset = pl.multiple_of(start + partner * width, LANES)
    moves = []
    for r in range(0, depth, rows):
        moves.append((up_src.at[r:r + rows], (rows, width), [((0, rows), (0, width), up_full.at[r:r + rows, pl.ds(offset, width)])]))
    for r in range(0, width, rows):
        size = min(rows, width - r)
        moves.append((down_src.at[r:r + size], (size, depth), [((0, size), (0, depth), down_full.at[pl.ds(offset + r, size)])]))
    return moves


def shared_moves(start, shared, packed, up_full, down_full):
    depth = up_full.shape[0]
    moves = []
    for device in range(packed.shape[0]):
        at = start + device * shared
        moves.append((packed.at[device, 0:shared], (shared, depth), [((0, shared), (0, depth), down_full.at[at:at + shared])]))
        parts = [((0, shared), (j * shared, shared), up_full.at[j * shared:(j + 1) * shared, at:at + shared]) for j in range(depth // shared)]
        moves.append((packed.at[device, shared:2 * shared], (shared, depth), parts))
    return moves


def move_load(move, ring, in_sem, slot):
    src, (height, width), _ = move
    return pltpu.make_async_copy(src, ring.at[slot, 0:height, 0:width], in_sem.at[slot])


def move_stores(move, ring, out_sem, slot):
    return [pltpu.make_async_copy(ring.at[slot, r0:r0 + rn, c0:c0 + cn], dst, out_sem.at[slot, p]) for p, ((r0, rn), (c0, cn), dst) in enumerate(move[2])]


def ffn_grad_kernel(blocks, steps, chunk, scale, background, ids, w_ref, dg_ref, h_ref, do_ref, *rest):
    if background is not None:
        shared_part, _, group = background
        packed = rest[0]
        rest = rest[3:]
        ring, in_sem, out_sem = rest[-3:]
        rest = rest[:-3]
    (up_full, down_full, up_send, down_send, w_t, g_s, d_s, acc_up, acc_down, sems) = rest
    i, t = pl.program_id(0), pl.program_id(1)
    block, tile = g_s.shape
    slot = lax.rem(i, 2)
    up_acc, down_acc = acc_up.at[slot], acc_down.at[slot]

    def copies(index, first=0, last=4):
        side = lax.rem(index, 2)
        full = pl.multiple_of(ids[1] + index * block, LANES)
        send = pl.multiple_of(index * block, LANES)
        pairs = (
            (acc_up.at[side], up_full.at[:, pl.ds(full, block)]),
            (acc_up.at[side], up_send.at[:, pl.ds(send, block)]),
            (acc_down.at[side], down_full.at[pl.ds(full, block)]),
            (acc_down.at[side], down_send.at[pl.ds(send, block)]),
        )
        return [pltpu.make_async_copy(*pairs[n], sems.at[side, n]) for n in range(first, last)]

    if background is not None:
        moves = shared_moves(*shared_part, packed, up_full, down_full)
        groups = [list(range(first, min(first + group, len(moves)))) for first in range(0, len(moves), group)]

        def load(n):
            return move_load(moves[n], ring, in_sem, n % (2 * group))

        def stores(n):
            return move_stores(moves[n], ring, out_sem, n % (2 * group))

        for step in range(steps):
            @pl.when(t == step)
            def _(step=step):
                if 0 <= step - 1 < len(groups):
                    for n in groups[step - 1]:
                        load(n).wait()
                        for store in stores(n):
                            store.start()
                if 0 <= step - 2 < len(groups):
                    for n in groups[step - 2]:
                        for store in stores(n):
                            store.wait()
                if step < len(groups):
                    for n in groups[step]:
                        load(n).start()

    @pl.when(t == 0)
    def _():
        w_t[:] = w_ref[:].T
        if blocks > 2:
            @pl.when(i >= 2)
            def _():
                for copy in copies(i - 2):
                    copy.wait()
        up_acc[:] = jnp.zeros(up_acc.shape, f32)
        down_acc[:] = jnp.zeros(down_acc.shape, f32)

    for j in range(tile // chunk):
        s = pl.ds(j * chunk, chunk)
        gated, d_up = gelu_pair(dot(w_t[:], h_ref[s, :], NT), dg_ref[:, s].astype(f32))
        g_s[:, s] = gated.astype(bf16)
        d_s[:, s] = d_up.astype(bf16)
    down_acc[:] += dot(g_s[:], do_ref[:], NN)

    @pl.when(t == steps - 1)
    def _():
        down_acc[:] = down_acc[:] * scale
        for copy in copies(i, first=2):
            copy.start()

    up_acc[:] += dot(h_ref[:], d_s[:], TT)

    @pl.when(t == steps - 1)
    def _():
        up_acc[:] = up_acc[:] * scale
        for copy in copies(i, last=2):
            copy.start()

        @pl.when(i == blocks - 1)
        def _():
            if background is not None:
                for group_at in range(max(0, steps - 2), len(groups)):
                    for n in groups[group_at]:
                        for store in stores(n):
                            store.wait()
            if blocks > 1:
                for copy in copies(i - 1):
                    copy.wait()
            for copy in copies(i):
                copy.wait()


def ffn_grad(ids, w_up, dg, hidden, d_out, ffn_width, width, block, tile, chunk, scale, background=None, sources=(), full=None):
    depth, rows = w_up.shape[0], hidden.shape[0]
    steps, blocks = rows // tile, width // block
    slots = min(blocks, 2)
    tile_spec = pl.BlockSpec((tile, depth), lambda i, t, ids: (t, 0))
    any_spec = pl.BlockSpec(memory_space=pl.ANY)
    weight_mode = {} if blocks > 1 else {'pipeline_mode': pl.Buffered(1)}
    in_specs = [pl.BlockSpec((depth, block), lambda i, t, ids: (0, ids[0] + i), **weight_mode), pl.BlockSpec((block, tile), lambda i, t, ids: (i, t)), tile_spec, tile_spec]
    operands = [ids, w_up, dg, hidden, d_out]
    aliases = {}
    scratch = [pltpu.VMEM((block, depth), bf16), pltpu.VMEM((block, tile), bf16), pltpu.VMEM((block, tile), bf16), pltpu.VMEM((slots, depth, block), f32), pltpu.VMEM((slots, block, depth), f32)]
    out_shape = [jax.ShapeDtypeStruct(shape, f32) for shape in ((depth, ffn_width), (ffn_width, depth), (depth, width), (width, depth))]
    scratch.append(pltpu.SemaphoreType.DMA((2, 4)))
    if background is not None:
        (_, shared), move_rows, group = background
        parts = depth // shared
        in_specs += [any_spec] * 3
        operands += [*sources, *full]
        aliases = {6: 0, 7: 1}
        scratch += [pltpu.VMEM((2 * group, move_rows, depth), f32), pltpu.SemaphoreType.DMA((2 * group,)), pltpu.SemaphoreType.DMA((2 * group, parts))]
    return pl.pallas_call(
        functools.partial(ffn_grad_kernel, blocks, steps, chunk, scale, background),
        grid_spec=pltpu.PrefetchScalarGridSpec(num_scalar_prefetch=1, grid=(blocks, steps), in_specs=in_specs, out_specs=[any_spec] * 4, scratch_shapes=scratch),
        out_shape=out_shape,
        input_output_aliases=aliases,
        compiler_params=params(2, 63),
        cost_estimate=pl.CostEstimate(flops=6 * width * depth * rows, bytes_accessed=2 * (width * depth + 2 * rows * depth + width * rows) + 16 * width * depth, transcendentals=width * rows),
        name='ffn_grad',
    )(*operands)


def assemble_kernel(part, slots, rows, ids, up_src, down_src, up_in, down_in, up_full, down_full, ring, in_sem, out_sem):
    moves = partner_moves(*part, rows, ids[0], up_src, down_src, up_full, down_full)

    def load(n):
        return move_load(moves[n], ring, in_sem, n % slots)

    def stores(n):
        return move_stores(moves[n], ring, out_sem, n % slots)

    ahead = slots // 2
    for n in range(min(ahead, len(moves))):
        load(n).start()
    for n in range(len(moves)):
        later = n + ahead
        if later < len(moves):
            if later >= slots:
                for copy in stores(later - slots):
                    copy.wait()
            load(later).start()
        load(n).wait()
        for copy in stores(n):
            copy.start()
    for n in range(max(0, len(moves) - slots), len(moves)):
        for copy in stores(n):
            copy.wait()


def assemble(partner, part, sources, full, slots=16, rows=256):
    any_spec = pl.BlockSpec(memory_space=pl.ANY)
    operands = [*sources, *full]
    depth = full[0].shape[0]
    return pl.pallas_call(
        functools.partial(assemble_kernel, part, slots, rows),
        grid_spec=pltpu.PrefetchScalarGridSpec(
            num_scalar_prefetch=1,
            grid=(),
            in_specs=[any_spec] * len(operands),
            out_specs=[any_spec] * 2,
            scratch_shapes=[pltpu.VMEM((slots, rows, depth), f32), pltpu.SemaphoreType.DMA((slots,)), pltpu.SemaphoreType.DMA((slots, 1))],
        ),
        out_shape=[jax.ShapeDtypeStruct(a.shape, f32) for a in full],
        input_output_aliases={len(operands) - 1: 0, len(operands): 1},
        compiler_params=pltpu.CompilerParams(vmem_limit_bytes=60 * MIB),
        cost_estimate=pl.CostEstimate(flops=0, bytes_accessed=8 * full[0].size // 8, transcendentals=0),
        name='assemble',
    )(partner, *operands)


def solution(mesh):
    cp_size = mesh.shape['cp']
    dp_size = mesh.shape['dp']
    device_count = dp_size * cp_size
    inv_div = 1.0 / device_count
    axis_perm = {
        'core': ('cp', [(source, source ^ 1) for source in range(cp_size)]),
        'x': ('cp', [(source, source ^ 2) for source in range(cp_size)]),
        'y': ('dp', [(source, source ^ 1) for source in range(dp_size)]),
        'z': ('dp', [(source, source ^ 2) for source in range(dp_size)]),
    }
    colour_axes = (('x', 'y', 'z'), ('y', 'z', 'x'), ('z', 'x', 'y'))

    def swap(value, axis):
        name, perm = axis_perm[axis]
        return lax.ppermute(value, name, perm)

    def bits_of(device):
        return {'z': device >> 3 & 1, 'y': device >> 2 & 1, 'x': device >> 1 & 1, 'core': device & 1}

    unit_of = []
    for device in range(device_count):
        bits = bits_of(device)
        for colour, axes in enumerate(colour_axes):
            unit_of.append((device, colour, 24 * bits['core'] + 8 * colour + 4 * bits[axes[0]] + 2 * bits[axes[1]] + bits[axes[2]]))

    def device_backward(x_in, d_out, w_q, w_k, w_v, w_o, w_up, w_down):
        batch_dev, seq_dev, depth = x_in.shape
        ffn_width = w_up.shape[1]
        heads, kv_heads, head_dim = w_q.shape[1], w_k.shape[1], w_k.shape[2]
        q_width, kv_width = heads * head_dim, kv_heads * head_dim
        score_scale = head_dim ** -0.5
        row_count = batch_dev * seq_dev
        x_rows = x_in.reshape(row_count, depth)
        dout_rows = d_out.reshape(row_count, depth)
        device = lax.axis_index('dp') * cp_size + lax.axis_index('cp')
        bits = bits_of(device)
        core = bits['core']
        phases = ((0, 1536, 512, 2048), (7168, 896, 896, 1024))
        shared_start, shared = 3072, 256

        dout_all = lax.all_gather(dout_rows, ('dp', 'cp'), axis=0, tiled=True)
        w_kv = jnp.concatenate([w_k.reshape(depth, kv_width), w_v.reshape(depth, kv_width)], axis=1)
        kv_own = dot(x_rows, w_kv, NN).astype(bf16)
        kv_far = swap(kv_own, 'x')
        kv_all = jnp.concatenate([kv_own, swap(kv_own, 'core'), kv_far, swap(kv_far, 'core')], axis=0)
        w_q_heads = w_q.transpose(1, 0, 2)
        w_o_rows = w_o.reshape(q_width, depth)
        q_own = q_proj(x_rows, w_q_heads)
        dg_own = own_gate(dout_rows, w_down, 1792)
        attn_out, lse = attn_fwd(q_own, kv_all, heads, kv_heads, head_dim, score_scale * LOG2E)
        hidden_rows = (x_rows.astype(f32) + dot(attn_out, w_o_rows, NN)).astype(bf16)
        hidden_all = lax.all_gather(hidden_rows, ('dp', 'cp'), axis=0, tiled=True)

        d_hidden = own_mlp(hidden_rows, dout_rows, dg_own, w_up, 1792, 7)
        d_attn = dot(d_hidden, w_o_rows, NT).astype(bf16)
        d_q, dk_part, dv_part = attn_bwd(q_own, kv_all, attn_out, d_attn, lse, heads, kv_heads, head_dim, score_scale * LOG2E, score_scale)
        dkv_part = jnp.concatenate([dk_part, dv_part], axis=1).reshape(2, 2, seq_dev, 2 * kv_width)
        dkv_pair = dkv_part[:, 0] + swap(dkv_part[:, 1], 'core')
        d_kv = (dkv_pair[0] + swap(dkv_pair[1], 'x')).astype(bf16)

        rhs = jnp.concatenate([d_q, d_kv, d_hidden], axis=1)

        def index(value):
            return jnp.reshape(value.astype(jnp.int32), (1,))

        keep, give = attn_wgrad(index(core), x_rows, attn_out, rhs, (q_width + 2 * kv_width) // (2 * LANES), inv_div)
        recv = swap(give, 'core')
        d_x = d_input(d_hidden, d_kv, w_kv, d_q, w_q_heads).reshape(batch_dev, seq_dev, depth)

        base_s = shared_start // shared + device
        dg_s = d_gate(index(base_s), w_down, dout_all, shared, shared, 2048)
        start_b, width_b, block_b, _ = phases[1]
        dg_b = d_gate(index(start_b // block_b + core), w_down, dout_all, width_b, block_b, 2048)
        packed, halves = shared_grad(w_up, dg_s, hidden_all, dout_all, keep, recv, (shared, shared_start // shared), 1024, 512, inv_div, colour_axes)
        dg_a, own_sum = gate_reduce(w_down, dout_all, halves, (512, 3, 0), 1024, colour_axes)
        packed_all = lax.all_gather(packed, ('dp', 'cp'), axis=0)
        summed = lax.all_gather(own_sum, ('dp', 'cp'), axis=0)
        splits = (heads // 2, heads // 2 + 2)
        dw_q, dw_k, dw_v, dw_o = attn_unpack(summed, unit_of, splits, depth)

        def ids_of(*values):
            return jnp.concatenate([index(value) for value in values])

        partner = 1 - core
        (start_a, width_a, block_a, tile_a), (start_b, width_b, block_b, tile_b) = phases
        up_full, down_full, up_send, down_send = ffn_grad(ids_of(start_a // block_a + core * (width_a // block_a), start_a + core * width_a), w_up, dg_a, hidden_all, dout_all, ffn_width, width_a, block_a, tile_a, 1024, inv_div)
        received_a = (swap(up_send, 'core'), swap(down_send, 'core'))
        background = ((shared_start, shared), shared, 5)
        up_full, down_full, up_send, down_send = ffn_grad(ids_of(start_b // block_b + core, start_b + core * width_b), w_up, dg_b, hidden_all, dout_all, ffn_width, width_b, block_b, tile_b, 512, inv_div, background, (packed_all,), (up_full, down_full))
        received_b = (swap(up_send, 'core'), swap(down_send, 'core'))
        full = assemble(index(partner), (start_a, width_a), received_a, (up_full, down_full))
        dw_up, dw_down = assemble(index(partner), (start_b, width_b), received_b, full)
        return d_x, dw_q.transpose(1, 0, 2), dw_k, dw_v, dw_o.reshape(w_o.shape), dw_up, dw_down

    act_spec = P('dp', 'cp', None)
    return jax.shard_map(device_backward, mesh=mesh, in_specs=(act_spec, act_spec, P(), P(), P(), P(), P(), P()), out_specs=(act_spec, P(), P(), P(), P(), P(), P()), check_vma=False)
```

```python
import functools
import jax
import jax.numpy as jnp
from jax import lax
from jax.experimental import pallas as pl
from jax.experimental.pallas import tpu as pltpu
from jax.sharding import PartitionSpec as P

f32, bf16 = jnp.float32, jnp.bfloat16
NN = (((1,), (0,)), ((), ()))
NT = (((1,), (1,)), ((), ()))
TN = (((0,), (0,)), ((), ()))
TT = (((0,), (1,)), ((), ()))
LOG2E = 1.4426950408889634
GELU_A = 0.7978845608028654
GELU_B = GELU_A * 0.044715
MIB = 1 << 20
LANES = 128
UNIT_ROWS = 32


def dot(a, b, dims):
    return lax.dot_general(a, b, dims, preferred_element_type=f32)


def params(rank, vmem):
    return pltpu.CompilerParams(dimension_semantics=('arbitrary',) * rank, vmem_limit_bytes=vmem * MIB)


def over_rows(ref, update, step=64):
    @pl.loop(0, ref.shape[0] // step)
    def _(i):
        rows = pl.ds(pl.multiple_of(i * step, step), step)
        ref[rows, :] = update(ref[rows, :])


def clear(ref):
    over_rows(ref, jnp.zeros_like)


def resident(shape):
    return pl.BlockSpec(shape, lambda *ids: (0,) * len(shape), pipeline_mode=pl.Buffered(1))


def attn_fwd_kernel(heads_step, coef, head_dim, q_ref, k_ref, v_ref, a_ref, l_ref):
    for i in range(heads_step):
        cols = slice(i * head_dim, (i + 1) * head_dim)
        scores = dot(k_ref[:], q_ref[:, cols], NT)
        top = jnp.max(scores, axis=0, keepdims=True)
        probs = jnp.exp2((scores - top) * coef)
        total = jnp.sum(probs, axis=0, keepdims=True)
        out_t = dot(v_ref[:], probs.astype(bf16), TN)
        a_ref[:, cols] = (out_t * (1.0 / total)).T.astype(bf16)
        l_ref[i] = jnp.broadcast_to(top * coef + jnp.log2(total), l_ref.shape[1:])


def attn_fwd(q, kv, heads, kv_heads, head_dim, coef):
    rows, keys = q.shape[0], kv.shape[0]
    step = heads // kv_heads // 2
    per = heads // kv_heads // step
    q_spec = pl.BlockSpec((rows, step * head_dim), lambda h: (0, h))
    return pl.pallas_call(
        functools.partial(attn_fwd_kernel, step, coef, head_dim),
        grid=(heads // step,),
        in_specs=[q_spec, pl.BlockSpec((keys, head_dim), lambda h: (0, h // per)), pl.BlockSpec((keys, head_dim), lambda h: (0, kv_heads + h // per))],
        out_specs=[q_spec, pl.BlockSpec((step, 8, rows), lambda h: (h, 0, 0))],
        out_shape=[jax.ShapeDtypeStruct(q.shape, bf16), jax.ShapeDtypeStruct((heads, 8, rows), f32)],
        compiler_params=params(1, 60),
        cost_estimate=pl.CostEstimate(flops=8 * rows * keys * head_dim * heads, bytes_accessed=8 * MIB, transcendentals=rows * keys * heads),
        name='attn_fwd',
    )(q, kv, kv)


def attn_bwd_kernel(heads_step, steps, coef, scale, head_dim, q_ref, k_ref, v_ref, a_ref, da_ref, l_ref, dq_ref, dk_ref, dv_ref):
    @pl.when(pl.program_id(1) == 0)
    def _():
        dk_ref[:] = jnp.zeros_like(dk_ref)
        dv_ref[:] = jnp.zeros_like(dv_ref)

    for i in range(heads_step):
        cols = slice(i * head_dim, (i + 1) * head_dim)
        q, da = q_ref[:, cols], da_ref[:, cols]
        delta = jnp.sum((da.astype(f32) * a_ref[:, cols].astype(f32)).T, axis=0, keepdims=True)
        probs = jnp.exp2(dot(k_ref[:], q, NT) * coef - l_ref[i, 0:1, :])
        d_probs = dot(v_ref[:], da, NT)
        d_scores = (probs * (d_probs - delta)).astype(bf16)
        dv_ref[:] += dot(probs.astype(bf16), da, NN)
        dk_ref[:] += dot(d_scores, q, NN)
        dq_ref[:, cols] = (dot(k_ref[:], d_scores, TN) * scale).T.astype(bf16)

    @pl.when(pl.program_id(1) == steps - 1)
    def _():
        dk_ref[:] = dk_ref[:] * scale


def attn_bwd(q, kv, a, da, lse, heads, kv_heads, head_dim, coef, scale):
    rows, keys = q.shape[0], kv.shape[0]
    step = heads // kv_heads // 2
    steps = heads // kv_heads // step
    q_spec = pl.BlockSpec((rows, step * head_dim), lambda g, h: (0, g * steps + h))
    kv_spec = pl.BlockSpec((keys, head_dim), lambda g, h: (0, g))
    kv_shape = jax.ShapeDtypeStruct((keys, kv_heads * head_dim), f32)
    return pl.pallas_call(
        functools.partial(attn_bwd_kernel, step, steps, coef, scale, head_dim),
        grid=(kv_heads, steps),
        in_specs=[q_spec, kv_spec, pl.BlockSpec((keys, head_dim), lambda g, h: (0, kv_heads + g)), q_spec, q_spec, pl.BlockSpec((step, 8, rows), lambda g, h: (g * steps + h, 0, 0))],
        out_specs=[q_spec, kv_spec, kv_spec],
        out_shape=[jax.ShapeDtypeStruct(q.shape, bf16), kv_shape, kv_shape],
        compiler_params=params(2, 62),
        cost_estimate=pl.CostEstimate(flops=14 * rows * keys * head_dim * heads, bytes_accessed=16 * MIB, transcendentals=rows * keys * heads),
        name='attn_bwd',
    )(q, kv, kv, a, da, lse)


def gelu_pair(u, d_gated):
    square = u * u
    a = 0.5 * jnp.tanh(u * (GELU_A + GELU_B * square)) + 0.5
    gated = u * a
    slope = a + (gated - gated * a) * (2 * GELU_A + (6 * GELU_B) * square)
    return gated, slope * d_gated


def side_by_side(w_ref):
    return jnp.concatenate([w_ref[j] for j in range(w_ref.shape[0])], axis=1)


def q_proj_kernel(x_ref, w_ref, o_ref):
    o_ref[:] = dot(x_ref[:], side_by_side(w_ref), NN).astype(bf16)


def q_proj(x, w_heads, step=4):
    rows, depth = x.shape
    heads, _, head_dim = w_heads.shape
    return pl.pallas_call(
        q_proj_kernel,
        grid=(heads // step,),
        in_specs=[pl.BlockSpec((rows, depth), lambda i: (0, 0)), pl.BlockSpec((step, depth, head_dim), lambda i: (i, 0, 0))],
        out_specs=pl.BlockSpec((rows, step * head_dim), lambda i: (0, i)),
        out_shape=jax.ShapeDtypeStruct((rows, heads * head_dim), bf16),
        compiler_params=params(1, 60),
        cost_estimate=pl.CostEstimate(flops=2 * rows * depth * heads * head_dim, bytes_accessed=8 * MIB, transcendentals=0),
        name='q_proj',
    )(x, w_heads)


def d_input_kernel(steps, dh_ref, dkv_ref, wkv_ref, dq_ref, w_ref, o_ref, acc):
    i = pl.program_id(0)

    @pl.when(i == 0)
    def _():
        acc[:] = dh_ref[:].astype(f32) + dot(dkv_ref[:], wkv_ref[:], NT)

    acc[:] += dot(dq_ref[:], side_by_side(w_ref), NT)

    @pl.when(i == steps - 1)
    def _():
        o_ref[:] = acc[:].astype(bf16)


def d_input(d_hidden, d_kv, w_kv, d_q, w_heads, step=4):
    rows, depth = d_hidden.shape
    heads, _, head_dim = w_heads.shape
    whole = lambda array: pl.BlockSpec(array.shape, lambda i: (0, 0))
    return pl.pallas_call(
        functools.partial(d_input_kernel, heads // step),
        grid=(heads // step,),
        in_specs=[whole(d_hidden), whole(d_kv), whole(w_kv), pl.BlockSpec((rows, step * head_dim), lambda i: (0, i)), pl.BlockSpec((step, depth, head_dim), lambda i: (i, 0, 0))],
        out_specs=whole(d_hidden),
        out_shape=jax.ShapeDtypeStruct((rows, depth), bf16),
        scratch_shapes=[pltpu.VMEM((rows, depth), f32)],
        compiler_params=params(1, 60),
        cost_estimate=pl.CostEstimate(flops=2 * rows * depth * heads * head_dim, bytes_accessed=12 * MIB, transcendentals=0),
        name='d_input',
    )(d_hidden, d_kv, w_kv, d_q, w_heads)


def own_gate_kernel(do_ref, wd_ref, o_ref):
    o_ref[:] = dot(do_ref[:], wd_ref[:], NT).astype(bf16)


def own_gate(d_out, w_down, block):
    rows, depth = d_out.shape
    width = w_down.shape[0]
    return pl.pallas_call(
        own_gate_kernel,
        grid=(width // block,),
        in_specs=[pl.BlockSpec((rows, depth), lambda i: (0, 0)), pl.BlockSpec((block, depth), lambda i: (i, 0))],
        out_specs=pl.BlockSpec((rows, block), lambda i: (0, i)),
        out_shape=jax.ShapeDtypeStruct((rows, width), bf16),
        compiler_params=params(1, 60),
        cost_estimate=pl.CostEstimate(flops=2 * rows * width * depth, bytes_accessed=2 * width * (depth + rows), transcendentals=0),
        name='own_gate',
    )(d_out, w_down)


def own_mlp_kernel(steps, parts, h_ref, do_ref, dg_ref, wu_ref, o_ref, acc):
    i = pl.program_id(0)

    @pl.when(i == 0)
    def _():
        acc[:] = do_ref[:].astype(f32)

    width = wu_ref.shape[1] // parts
    d_up = []
    for j in range(parts):
        cols = slice(j * width, (j + 1) * width)
        up = dot(h_ref[:], wu_ref[:, cols], NN)
        d_up.append(gelu_pair(up, dg_ref[:, cols].astype(f32))[1].astype(bf16))
    acc[:] += dot(jnp.concatenate(d_up, axis=1), wu_ref[:], NT)

    @pl.when(i == steps - 1)
    def _():
        o_ref[:] = acc[:].astype(bf16)


def own_mlp(hidden, d_out, dg, w_up, block, parts):
    rows, depth = hidden.shape
    width = w_up.shape[1]
    full = pl.BlockSpec((rows, depth), lambda i: (0, 0))
    return pl.pallas_call(
        functools.partial(own_mlp_kernel, width // block, parts),
        grid=(width // block,),
        in_specs=[full, full, pl.BlockSpec((rows, block), lambda i: (0, i)), pl.BlockSpec((depth, block), lambda i: (0, i))],
        out_specs=full,
        out_shape=jax.ShapeDtypeStruct((rows, depth), bf16),
        scratch_shapes=[pltpu.VMEM((rows, depth), f32)],
        compiler_params=params(1, 60),
        cost_estimate=pl.CostEstimate(flops=4 * rows * width * depth, bytes_accessed=2 * width * (depth + rows), transcendentals=rows * width),
        name='own_mlp',
    )(hidden, d_out, dg, w_up)


def attn_wgrad_kernel(kv_end, scale, ids, x_ref, a_ref, rhs_ref, keep_ref, give_ref, xt, at):
    i = pl.program_id(0)

    @pl.when(i == 0)
    def _():
        xt[:] = x_ref[:].T
        at[:] = a_ref[:].T

    half = xt.shape[0] // 2

    def emit(lhs):
        for side, target in ((ids[0], keep_ref), (1 - ids[0], give_ref)):
            product = dot(lhs[pl.ds(pl.multiple_of(side * half, UNIT_ROWS), half), :], rhs_ref[:], NN) * scale
            for j in range(target.shape[1]):
                target[:, j] = product[:, j * LANES:(j + 1) * LANES].reshape(target.shape[0], UNIT_ROWS, LANES)

    @pl.when(i < kv_end)
    def _():
        emit(xt)

    @pl.when(i >= kv_end)
    def _():
        emit(at)


def attn_wgrad(core, x, a, rhs, kv_end, scale, slabs=4):
    rows, depth = x.shape
    width = rhs.shape[1]
    units = depth // UNIT_ROWS // 2
    full = pl.BlockSpec((rows, depth), lambda i, ids: (0, 0))
    out_spec = pl.BlockSpec((units, slabs, UNIT_ROWS, LANES), lambda i, ids: (0, i, 0, 0))
    return pl.pallas_call(
        functools.partial(attn_wgrad_kernel, kv_end, scale),
        grid_spec=pltpu.PrefetchScalarGridSpec(
            num_scalar_prefetch=1,
            grid=(width // (slabs * LANES),),
            in_specs=[full, full, pl.BlockSpec((rows, slabs * LANES), lambda i, ids: (0, i))],
            out_specs=[out_spec, out_spec],
            scratch_shapes=[pltpu.VMEM((depth, rows), bf16), pltpu.VMEM((depth, rows), bf16)],
        ),
        out_shape=[jax.ShapeDtypeStruct((units, width // LANES, UNIT_ROWS, LANES), f32)] * 2,
        compiler_params=params(1, 60),
        cost_estimate=pl.CostEstimate(flops=2 * rows * width * depth, bytes_accessed=4 * width * depth, transcendentals=0),
        name='attn_wgrad',
    )(core, x, a, rhs)


def attn_unpack_kernel(unit_of, splits, in_ref, q_ref, k_ref, v_ref, o_ref):
    i = pl.program_id(0)
    first, second = splits

    def each(store):
        for device, colour, unit in unit_of:
            for j in range(in_ref.shape[2]):
                store(slice(unit * UNIT_ROWS, (unit + 1) * UNIT_ROWS), j, in_ref[device, colour, j])

    @pl.when(i < first)
    def _():
        def store(rows, j, value):
            q_ref[j, rows] = value

        each(store)

    @pl.when((i >= first) & (i < second))
    def _():
        def store(rows, j, value):
            o_ref[rows, j * LANES:(j + 1) * LANES] = value

        each(store)

    @pl.when(i >= second)
    def _():
        def store(rows, j, value):
            (k_ref, v_ref)[j // 2][rows, j % 2] = value

        each(store)


def attn_unpack(gathered, unit_of, splits, depth, step=4):
    devices, colours, slabs = gathered.shape[:3]
    first, second = splits
    kv_spec = pl.BlockSpec((depth, 2, LANES), lambda i: (0, 0, 0), pipeline_mode=pl.Buffered(1))
    kv_shape = jax.ShapeDtypeStruct((depth, 2, LANES), f32)
    return pl.pallas_call(
        functools.partial(attn_unpack_kernel, unit_of, splits),
        grid=(slabs // step,),
        in_specs=[pl.BlockSpec((devices, colours, step, UNIT_ROWS, LANES), lambda i: (0, 0, i, 0, 0))],
        out_specs=[
            pl.BlockSpec((step, depth, LANES), lambda i: (jnp.minimum(i, first - 1), 0, 0)),
            kv_spec,
            kv_spec,
            pl.BlockSpec((depth, step * LANES), lambda i: (0, jnp.clip(i - first, 0, second - first - 1))),
        ],
        out_shape=[jax.ShapeDtypeStruct((step * first, depth, LANES), f32), kv_shape, kv_shape, jax.ShapeDtypeStruct((depth, step * (second - first) * LANES), f32)],
        compiler_params=params(1, 60),
        cost_estimate=pl.CostEstimate(flops=0, bytes_accessed=2 * gathered.size * 4, transcendentals=0),
        name='attn_unpack',
    )(gathered)


def d_gates_kernel(count, ids, *refs):
    d_out = refs[count]
    for n in range(count):
        refs[count + 1 + n][:] = dot(refs[n][:], d_out[:], NT).astype(bf16)


def d_gates(bases, weights, heights, totals, d_out, tile):
    rows, depth = d_out.shape
    count = len(weights)

    def weight_spec(n):
        return pl.BlockSpec((heights[n], depth), lambda t, ids: (ids[n], 0), pipeline_mode=pl.Buffered(1))

    return pl.pallas_call(
        functools.partial(d_gates_kernel, count),
        grid_spec=pltpu.PrefetchScalarGridSpec(
            num_scalar_prefetch=1,
            grid=(rows // tile,),
            in_specs=[weight_spec(n) for n in range(count)] + [pl.BlockSpec((tile, depth), lambda t, ids: (t, 0))],
            out_specs=[pl.BlockSpec((height, tile), lambda t, ids: (0, t)) for height in heights],
        ),
        out_shape=[jax.ShapeDtypeStruct((total, rows), bf16) for total in totals],
        compiler_params=params(1, 60),
        cost_estimate=pl.CostEstimate(flops=2 * sum(heights) * depth * rows, bytes_accessed=2 * rows * (depth + sum(heights)), transcendentals=0),
        name='d_gates',
    )(bases, *weights, d_out)


def mesh_bits():
    dp, cp = lax.axis_index('dp'), lax.axis_index('cp')
    return dp, cp, {'z': dp // 2, 'y': lax.rem(dp, 2), 'x': cp // 2, 'core': lax.rem(cp, 2)}


def neighbour(dp, cp, bits, axis):
    flip = 1 - 2 * bits[axis]
    return {'x': (dp, cp + 2 * flip), 'y': (dp + flip, cp), 'z': (dp + 2 * flip, cp)}[axis]


def rs_bit(bits, colour_axes, colour, level):
    return bits[colour_axes[colour][level]]


def greet(axes, dp, cp, bits):
    barrier = pltpu.get_barrier_semaphore()
    for axis in axes:
        pl.semaphore_signal(barrier, inc=1, device_id=neighbour(dp, cp, bits, axis), device_id_type=pl.DeviceIdType.MESH)
    pl.semaphore_wait(barrier, len(axes))


def transfer(src, dst, sems, at, target):
    return pltpu.make_async_remote_copy(src_ref=src, dst_ref=dst, send_sem=sems[0].at[at], recv_sem=sems[1].at[at], device_id=target, device_id_type=pl.DeviceIdType.MESH)


def gelu_tile(w_t, dg_ref, h_ref, g_s, d_s, chunk):
    for j in range(g_s.shape[1] // chunk):
        s = pl.ds(j * chunk, chunk)
        gated, d_up = gelu_pair(dot(w_t[:], h_ref[s, :], NT), dg_ref[:, s].astype(f32))
        g_s[:, s] = gated.astype(bf16)
        d_s[:, s] = d_up.astype(bf16)


def host_params(collective_id):
    return pltpu.CompilerParams(dimension_semantics=('arbitrary',), vmem_limit_bytes=63 * MIB, collective_id=collective_id, has_side_effects=True)


def shared_grad_kernel(split, chunk, scale, colour_axes, wd_ref, w_ref, dg_ref, h_ref, do_ref, keep_a, recv_a, keep_b, recv_b, gate_in, out_ref, mine, gate_ref, w_t, g_s, d_s, acc_up, acc_down, send, other, incoming, load_sem, *sems):
    t = pl.program_id(0)
    block = g_s.shape[0]
    dp, cp, bits = mesh_bits()
    colours = range(len(colour_axes))
    slabs = keep_a.shape[1]

    def loads(kind, colour):
        first = rs_bit(bits, colour_axes, colour, 0)
        side = first if kind % 2 else 1 - first
        units = pl.ds(8 * colour + 4 * side, 4)
        target = (send, mine, other, other)[kind]
        sources = ((keep_a, keep_b), (recv_a, recv_b))[kind // 2]
        for n, (source, part) in enumerate(zip(sources, (slice(slabs), slice(slabs, None)))):
            yield pltpu.make_async_copy(source.at[units], target.at[colour, :, part], load_sem.at[n, kind, colour])

    def start(kind, colour):
        for copy in loads(kind, colour):
            copy.start()

    def finish(kind, colour):
        for copy in loads(kind, colour):
            copy.wait()

    def exchange(colour):
        return transfer(send.at[colour], incoming.at[colour], sems, colour, neighbour(dp, cp, bits, colour_axes[colour][0]))

    @pl.when(t == 0)
    def _():
        for colour in colours:
            start(0, colour)
            start(2, colour)
        greet(('x', 'y', 'z'), dp, cp, bits)
        w_t[:] = w_ref[:].T
        for colour in colours:
            finish(0, colour)
            finish(2, colour)
            send[colour] = send[colour] + other[colour]
        for colour in colours:
            exchange(colour).start()
            start(1, colour)
            start(3, colour)
        clear(acc_up)
        clear(acc_down)

    @pl.when(t == 1)
    def _():
        for colour in colours:
            finish(1, colour)
            finish(3, colour)
            mine[colour] = mine[colour] + other[colour]

    @pl.when(t < split)
    def _():
        gelu_tile(w_t, dg_ref, h_ref, g_s, d_s, chunk)
        acc_down[:] += dot(g_s[:], do_ref[:], NN)
        acc_up[:] += dot(h_ref[:], d_s[:], TT)

    @pl.when(t == split)
    def _():
        out_ref[:block] = acc_down[:] * scale
        for j in range(acc_up.shape[0] // block):
            out_ref[block:, j * block:(j + 1) * block] = acc_up[j * block:(j + 1) * block, :] * scale

    @pl.when(t >= split)
    def _():
        gate_ref[:] = dot(wd_ref[:], do_ref[:], NT).astype(bf16)

    @pl.when(t == 2 * split - 1)
    def _():
        for colour in colours:
            exchange(colour).wait()
            mine[colour] = mine[colour] + incoming[colour]


def shared_grad(w_down, w_up, dg, hidden, d_out, sets, gated, shared, gate, tile, chunk, scale, colour_axes):
    block, base = shared
    gate_block, gate_count, gate_base = gate
    depth, rows = w_up.shape[0], hidden.shape[0]
    split, colours = rows // tile, len(colour_axes)
    (keep_a, _), (keep_b, _) = sets
    half = (colours, 4, keep_a.shape[1] + keep_b.shape[1]) + keep_a.shape[2:]
    any_spec = pl.BlockSpec(memory_space=pl.ANY)
    once = pl.Buffered(1)

    def device():
        return lax.axis_index('dp') * lax.axis_size('cp') + lax.axis_index('cp')

    def early(t):
        return jnp.minimum(t, split - 1)

    return pl.pallas_call(
        functools.partial(shared_grad_kernel, split, chunk, scale, colour_axes),
        grid=(2 * split,),
        in_specs=[
            pl.BlockSpec((gate_block, depth), lambda t: (gate_base + gate_count * lax.rem(lax.axis_index('cp'), 2) + 1, 0), pipeline_mode=once),
            pl.BlockSpec((depth, block), lambda t: (0, base + device()), pipeline_mode=once),
            pl.BlockSpec((block, tile), lambda t: (0, early(t))),
            pl.BlockSpec((tile, depth), lambda t: (early(t), 0)),
            pl.BlockSpec((tile, depth), lambda t: (t % split, 0)),
        ] + [any_spec] * 5,
        out_specs=[resident((2 * block, depth)), resident(half), pl.BlockSpec((gate_block, tile), lambda t: (1, jnp.maximum(t - split, 0)))],
        out_shape=[jax.ShapeDtypeStruct((2 * block, depth), f32), jax.ShapeDtypeStruct(half, f32), jax.ShapeDtypeStruct(gated.shape, bf16)],
        scratch_shapes=[
            pltpu.VMEM((block, depth), bf16), pltpu.VMEM((block, tile), bf16), pltpu.VMEM((block, tile), bf16), pltpu.VMEM((depth, block), f32), pltpu.VMEM((block, depth), f32),
            pltpu.VMEM(half, f32), pltpu.VMEM(half, f32), pltpu.VMEM(half, f32),
            pltpu.SemaphoreType.DMA((2, 4, colours)), pltpu.SemaphoreType.DMA((colours,)), pltpu.SemaphoreType.DMA((colours,)),
        ],
        input_output_aliases={9: 2},
        compiler_params=host_params(0),
        cost_estimate=pl.CostEstimate(flops=2 * depth * rows * (3 * block + gate_block), bytes_accessed=4 * rows * depth, transcendentals=block * rows),
        name='shared_grad',
    )(w_down, w_up, dg, hidden, d_out, *sets[0], *sets[1], gated)


def gate_reduce_kernel(split, steps, ready, chunk, scale, colour_axes, wd_ref, do_ref, w_ref, dg_ref, h_ref, mine, gate_in, gate_ref, up_ref, down_ref, sum_ref, w_t, g_s, d_s, rest, in2, in3, load_sem, *sems):
    s = pl.program_id(0)
    dp, cp, bits = mesh_bits()
    colours = range(len(colour_axes))

    def bit(colour, level):
        return rs_bit(bits, colour_axes, colour, level)

    def exchange(level, colour):
        if level == 1:
            src, dst = mine.at[colour, pl.ds(2 * (1 - bit(colour, 1)), 2)], in2.at[colour]
        else:
            src, dst = rest.at[colour, pl.ds(1 - bit(colour, 2), 1)], in3.at[colour]
        return transfer(src, dst, sems, (level - 1, colour), neighbour(dp, cp, bits, colour_axes[colour][level]))

    def load(colour):
        return pltpu.make_async_copy(mine.at[colour, pl.ds(2 * bit(colour, 1), 2)], rest.at[colour], load_sem.at[colour])

    @pl.when(s == 0)
    def _():
        greet(('x', 'y', 'z'), dp, cp, bits)
        for colour in colours:
            exchange(1, colour).start()
            load(colour).start()

    @pl.when(s == ready)
    def _():
        for colour in colours:
            exchange(1, colour).wait()
            load(colour).wait()
            rest[colour] = rest[colour] + in2[colour]
        for colour in colours:
            exchange(2, colour).start()

    @pl.when(s < split)
    def _():
        gate_ref[:] = dot(wd_ref[:], do_ref[:], NT).astype(bf16)

    @pl.when(s == split)
    def _():
        w_t[:] = w_ref[:].T
        clear(up_ref)
        clear(down_ref)

    @pl.when(s >= split)
    def _():
        gelu_tile(w_t, dg_ref, h_ref, g_s, d_s, chunk)
        down_ref[:] += dot(g_s[:], do_ref[:], NN)
        up_ref[:] += dot(h_ref[:], d_s[:], TT)

    @pl.when(s == steps - 1)
    def _():
        over_rows(up_ref, lambda value: value * scale)
        over_rows(down_ref, lambda value: value * scale)
        for colour in colours:
            exchange(2, colour).wait()
            sum_ref[colour] = rest[colour, bit(colour, 2)] + in3[colour, 0]


def gate_reduce(w_down, up_cols, d_out, dg, hidden, mine, gated, gate, tile, chunk, scale, colour_axes):
    gate_block, gate_count, gate_base = gate
    width = up_cols.shape[1]
    depth, rows = w_down.shape[1], d_out.shape[0]
    tiles = rows // tile
    split = tiles
    steps = split + tiles
    colours = len(colour_axes)
    slab = mine.shape[2:]
    any_spec = pl.BlockSpec(memory_space=pl.ANY)

    def core():
        return lax.rem(lax.axis_index('cp'), 2)

    def early(s):
        return jnp.minimum(s, split - 1)

    def late(s):
        return jnp.maximum(s - split, 0)

    return pl.pallas_call(
        functools.partial(gate_reduce_kernel, split, steps, split + split // 2, chunk, scale, colour_axes),
        grid=(steps,),
        in_specs=[
            pl.BlockSpec((gate_block, depth), lambda s: (gate_base + gate_count * core() + gate_count - 1, 0), pipeline_mode=pl.Buffered(1)),
            pl.BlockSpec((tile, depth), lambda s: (s % tiles, 0)),
            pl.BlockSpec((depth, width), lambda s: (0, 0), pipeline_mode=pl.Buffered(1)),
            pl.BlockSpec((width, tile), lambda s: (0, late(s))),
            pl.BlockSpec((tile, depth), lambda s: (late(s), 0)),
            any_spec,
            any_spec,
        ],
        out_specs=[pl.BlockSpec((gate_block, tile), lambda s: (gate_count - 1, early(s))), resident((depth, width)), resident((width, depth)), resident((colours,) + slab)],
        out_shape=[jax.ShapeDtypeStruct(gated.shape, bf16), jax.ShapeDtypeStruct((depth, width), f32), jax.ShapeDtypeStruct((width, depth), f32), jax.ShapeDtypeStruct((colours,) + slab, f32)],
        scratch_shapes=[
            pltpu.VMEM((width, depth), bf16), pltpu.VMEM((width, tile), bf16), pltpu.VMEM((width, tile), bf16),
            pltpu.VMEM((colours, 2) + slab, f32), pltpu.VMEM((colours, 2) + slab, f32), pltpu.VMEM((colours, 1) + slab, f32),
            pltpu.SemaphoreType.DMA((colours,)), pltpu.SemaphoreType.DMA((2, colours)), pltpu.SemaphoreType.DMA((2, colours)),
        ],
        input_output_aliases={6: 0},
        compiler_params=host_params(1),
        cost_estimate=pl.CostEstimate(flops=2 * depth * rows * (gate_block + 3 * width), bytes_accessed=100 * MIB, transcendentals=0),
        name='gate_reduce',
    )(w_down, d_out, up_cols, dg, hidden, mine, gated)


def partner_moves(start, width, rows, partner, up_src, down_src, up_full, down_full):
    depth = up_full.shape[0]
    offset = pl.multiple_of(start + partner * width, LANES)
    moves = []
    for r in range(0, depth, rows):
        moves.append((up_src.at[r:r + rows], (rows, width), [((0, rows), (0, width), up_full.at[r:r + rows, pl.ds(offset, width)])]))
    for r in range(0, width, rows):
        size = min(rows, width - r)
        moves.append((down_src.at[r:r + size], (size, depth), [((0, size), (0, depth), down_full.at[pl.ds(offset + r, size)])]))
    return moves


def shared_moves(start, shared, packed, up_full, down_full):
    depth = up_full.shape[0]
    moves = []
    for device in range(packed.shape[0]):
        at = start + device * shared
        moves.append((packed.at[device, 0:shared], (shared, depth), [((0, shared), (0, depth), down_full.at[at:at + shared])]))
        parts = [((0, shared), (j * shared, shared), up_full.at[j * shared:(j + 1) * shared, at:at + shared]) for j in range(depth // shared)]
        moves.append((packed.at[device, shared:2 * shared], (shared, depth), parts))
    return moves


def move_load(move, ring, in_sem, slot):
    src, (height, width), _ = move
    return pltpu.make_async_copy(src, ring.at[slot, 0:height, 0:width], in_sem.at[slot])


def move_stores(move, ring, out_sem, slot):
    return [pltpu.make_async_copy(ring.at[slot, r0:r0 + rn, c0:c0 + cn], dst, out_sem.at[slot, p]) for p, ((r0, rn), (c0, cn), dst) in enumerate(move[2])]


def ffn_grad_kernel(blocks, steps, chunk, scale, background, ids, w_ref, dg_ref, h_ref, do_ref, *rest):
    part, shared_part, rows, group, fresh = background
    up_src, down_src = rest[:2]
    packed = rest[2] if shared_part else None
    rest = rest[2 + bool(shared_part) + 2 * (not fresh):]
    (up_full, down_full, up_send, down_send, w_t, g_s, d_s, acc_up, acc_down, sems, ring, in_sem, out_sem) = rest
    i, t = pl.program_id(0), pl.program_id(1)
    now = i * steps + t
    block, _ = g_s.shape
    slot = lax.rem(i, 2)
    up_acc, down_acc = acc_up.at[slot], acc_down.at[slot]

    def copies(index, first=0, last=4):
        side = lax.rem(index, 2)
        full = pl.multiple_of(ids[1] + index * block, LANES)
        send = pl.multiple_of(index * block, LANES)
        pairs = (
            (acc_up.at[side], up_full.at[:, pl.ds(full, block)]),
            (acc_up.at[side], up_send.at[:, pl.ds(send, block)]),
            (acc_down.at[side], down_full.at[pl.ds(full, block)]),
            (acc_down.at[side], down_send.at[pl.ds(send, block)]),
        )
        return [pltpu.make_async_copy(*pairs[n], sems.at[side, n]) for n in range(first, last)]

    moves = partner_moves(*part, rows, ids[2], up_src, down_src, up_full, down_full)
    if shared_part:
        moves = moves + shared_moves(*shared_part, packed, up_full, down_full)
    assert len(moves) <= group * (blocks * steps - 1)
    groups = [list(range(first, min(first + group, len(moves)))) for first in range(0, len(moves), group)]

    def load(n):
        return move_load(moves[n], ring, in_sem, n % (2 * group))

    def stores(n):
        return move_stores(moves[n], ring, out_sem, n % (2 * group))

    for step in range(min(len(groups) + 2, blocks * steps)):
        @pl.when(now == step)
        def _(step=step):
            if 0 <= step - 1 < len(groups):
                for n in groups[step - 1]:
                    load(n).wait()
                    for store in stores(n):
                        store.start()
            if 0 <= step - 2 < len(groups):
                for n in groups[step - 2]:
                    for store in stores(n):
                        store.wait()
            if step < len(groups):
                for n in groups[step]:
                    load(n).start()

    @pl.when(t == 0)
    def _():
        w_t[:] = w_ref[:].T
        if blocks > 2:
            @pl.when(i >= 2)
            def _():
                for copy in copies(i - 2):
                    copy.wait()
        clear(up_acc)
        clear(down_acc)

    gelu_tile(w_t, dg_ref, h_ref, g_s, d_s, chunk)
    down_acc[:] += dot(g_s[:], do_ref[:], NN)
    up_acc[:] += dot(h_ref[:], d_s[:], TT)

    @pl.when(t == steps - 1)
    def _():
        over_rows(down_acc, lambda value: value * scale)
        for copy in copies(i, first=2):
            copy.start()
        over_rows(up_acc, lambda value: value * scale)
        for copy in copies(i, last=2):
            copy.start()

        @pl.when(i == blocks - 1)
        def _():
            for group_at in range(max(0, blocks * steps - 2), len(groups)):
                for n in groups[group_at]:
                    for store in stores(n):
                        store.wait()
            if blocks > 1:
                for copy in copies(i - 1):
                    copy.wait()
            for copy in copies(i):
                copy.wait()


def ffn_grad(ids, w_up, dg, hidden, d_out, ffn_width, width, block, tile, chunk, scale, background, sources, full=()):
    depth, rows = w_up.shape[0], hidden.shape[0]
    steps, blocks = rows // tile, width // block
    slots = min(blocks, 2)
    _, shared_part, move_rows, group = background
    tile_spec = pl.BlockSpec((tile, depth), lambda i, t, ids: (t, 0))
    any_spec = pl.BlockSpec(memory_space=pl.ANY)
    weight_mode = {} if blocks > 1 else {'pipeline_mode': pl.Buffered(1)}
    in_specs = [pl.BlockSpec((depth, block), lambda i, t, ids: (0, ids[0] + i), **weight_mode), pl.BlockSpec((block, tile), lambda i, t, ids: (i, t)), tile_spec, tile_spec]
    operands = [ids, w_up, dg, hidden, d_out, *sources, *full]
    in_specs += [any_spec] * (len(sources) + len(full))
    aliases = {len(operands) - len(full) + n: n for n in range(len(full))}
    parts = depth // shared_part[1] if shared_part else 1
    scratch = [
        pltpu.VMEM((block, depth), bf16), pltpu.VMEM((block, tile), bf16), pltpu.VMEM((block, tile), bf16), pltpu.VMEM((slots, depth, block), f32), pltpu.VMEM((slots, block, depth), f32),
        pltpu.SemaphoreType.DMA((2, 4)), pltpu.VMEM((2 * group, move_rows, depth), f32), pltpu.SemaphoreType.DMA((2 * group,)), pltpu.SemaphoreType.DMA((2 * group, parts)),
    ]
    out_shape = [jax.ShapeDtypeStruct(shape, f32) for shape in ((depth, ffn_width), (ffn_width, depth), (depth, width), (width, depth))]
    return pl.pallas_call(
        functools.partial(ffn_grad_kernel, blocks, steps, chunk, scale, (*background, not full)),
        grid_spec=pltpu.PrefetchScalarGridSpec(num_scalar_prefetch=1, grid=(blocks, steps), in_specs=in_specs, out_specs=[any_spec] * 4, scratch_shapes=scratch),
        out_shape=out_shape,
        input_output_aliases=aliases,
        compiler_params=params(2, 63),
        cost_estimate=pl.CostEstimate(flops=6 * width * depth * rows, bytes_accessed=2 * (width * depth + 2 * rows * depth + width * rows) + 16 * width * depth, transcendentals=width * rows),
        name='ffn_grad',
    )(*operands)


def assemble_kernel(part, slots, rows, ids, up_src, down_src, up_in, down_in, up_full, down_full, ring, in_sem, out_sem):
    moves = partner_moves(*part, rows, ids[0], up_src, down_src, up_full, down_full)

    def load(n):
        return move_load(moves[n], ring, in_sem, n % slots)

    def stores(n):
        return move_stores(moves[n], ring, out_sem, n % slots)

    ahead = slots // 2
    for n in range(min(ahead, len(moves))):
        load(n).start()
    for n in range(len(moves)):
        later = n + ahead
        if later < len(moves):
            if later >= slots:
                for copy in stores(later - slots):
                    copy.wait()
            load(later).start()
        load(n).wait()
        for copy in stores(n):
            copy.start()
    for n in range(max(0, len(moves) - slots), len(moves)):
        for copy in stores(n):
            copy.wait()


def assemble(partner, part, sources, full, slots=16, rows=256):
    any_spec = pl.BlockSpec(memory_space=pl.ANY)
    operands = [*sources, *full]
    depth = full[0].shape[0]
    return pl.pallas_call(
        functools.partial(assemble_kernel, part, slots, rows),
        grid_spec=pltpu.PrefetchScalarGridSpec(
            num_scalar_prefetch=1,
            grid=(),
            in_specs=[any_spec] * len(operands),
            out_specs=[any_spec] * 2,
            scratch_shapes=[pltpu.VMEM((slots, rows, depth), f32), pltpu.SemaphoreType.DMA((slots,)), pltpu.SemaphoreType.DMA((slots, 1))],
        ),
        out_shape=[jax.ShapeDtypeStruct(a.shape, f32) for a in full],
        input_output_aliases={len(operands) - 1: 0, len(operands): 1},
        compiler_params=pltpu.CompilerParams(vmem_limit_bytes=60 * MIB),
        cost_estimate=pl.CostEstimate(flops=0, bytes_accessed=8 * full[0].size // 8, transcendentals=0),
        name='assemble',
    )(partner, *operands)


def solution(mesh):
    cp_size = mesh.shape['cp']
    dp_size = mesh.shape['dp']
    device_count = dp_size * cp_size
    inv_div = 1.0 / device_count
    axis_perm = {
        'core': ('cp', [(source, source ^ 1) for source in range(cp_size)]),
        'x': ('cp', [(source, source ^ 2) for source in range(cp_size)]),
        'y': ('dp', [(source, source ^ 1) for source in range(dp_size)]),
        'z': ('dp', [(source, source ^ 2) for source in range(dp_size)]),
    }
    colour_axes = (('x', 'y', 'z'), ('y', 'z', 'x'), ('z', 'x', 'y'))

    def swap(value, axis):
        name, perm = axis_perm[axis]
        return lax.ppermute(value, name, perm)

    def bits_of(device):
        return {'z': device >> 3 & 1, 'y': device >> 2 & 1, 'x': device >> 1 & 1, 'core': device & 1}

    unit_of = []
    for device in range(device_count):
        bits = bits_of(device)
        for colour, axes in enumerate(colour_axes):
            unit_of.append((device, colour, 24 * bits['core'] + 8 * colour + 4 * bits[axes[0]] + 2 * bits[axes[1]] + bits[axes[2]]))

    def device_backward(x_in, d_out, w_q, w_k, w_v, w_o, w_up, w_down):
        batch_dev, seq_dev, depth = x_in.shape
        ffn_width = w_up.shape[1]
        heads, kv_heads, head_dim = w_q.shape[1], w_k.shape[1], w_k.shape[2]
        q_width, kv_width = heads * head_dim, kv_heads * head_dim
        score_scale = head_dim ** -0.5
        row_count = batch_dev * seq_dev
        x_rows = x_in.reshape(row_count, depth)
        dout_rows = d_out.reshape(row_count, depth)
        device = lax.axis_index('dp') * cp_size + lax.axis_index('cp')
        bits = bits_of(device)
        core = bits['core']
        start_a, width_a, block_a = 0, 1536, 512
        shared_start, shared = 3072, 256
        start_b, width_b = 7168, 512
        start_c, width_c = 8192, 384
        at_c = start_c + core * width_c

        dout_all = lax.all_gather(dout_rows, ('dp', 'cp'), axis=0, tiled=True)
        w_kv = jnp.concatenate([w_k.reshape(depth, kv_width), w_v.reshape(depth, kv_width)], axis=1)
        kv_own = dot(x_rows, w_kv, NN).astype(bf16)
        kv_far = swap(kv_own, 'x')
        kv_all = jnp.concatenate([kv_own, swap(kv_own, 'core'), kv_far, swap(kv_far, 'core')], axis=0)
        w_q_heads = w_q.transpose(1, 0, 2)
        w_o_rows = w_o.reshape(q_width, depth)
        q_own = q_proj(x_rows, w_q_heads)
        dg_own = own_gate(dout_rows, w_down, 1792)
        attn_out, lse = attn_fwd(q_own, kv_all, heads, kv_heads, head_dim, score_scale * LOG2E)
        hidden_rows = (x_rows.astype(f32) + dot(attn_out, w_o_rows, NN)).astype(bf16)
        hidden_all = lax.all_gather(hidden_rows, ('dp', 'cp'), axis=0, tiled=True)

        d_hidden = own_mlp(hidden_rows, dout_rows, dg_own, w_up, 1792, 7)
        d_attn = dot(d_hidden, w_o_rows, NT).astype(bf16)
        d_q, dk_part, dv_part = attn_bwd(q_own, kv_all, attn_out, d_attn, lse, heads, kv_heads, head_dim, score_scale * LOG2E, score_scale)

        def index(value):
            return jnp.reshape(value.astype(jnp.int32), (1,))

        dkv_part = jnp.concatenate([dk_part, dv_part], axis=1).reshape(2, 2, seq_dev, 2 * kv_width)
        dkv_other = swap(dkv_part[:, 1], 'core')
        keep, give = attn_wgrad(index(core), x_rows, attn_out, jnp.concatenate([d_q, d_hidden], axis=1), q_width // (4 * LANES), inv_div)
        recv = swap(give, 'core')
        dkv_pair = dkv_part[:, 0] + dkv_other
        d_kv = (dkv_pair[0] + swap(dkv_pair[1], 'x')).astype(bf16)
        keep_kv, give_kv = attn_wgrad(index(core), x_rows, attn_out, d_kv, 1, inv_div)
        recv_kv = swap(give_kv, 'core')
        d_x = d_input(d_hidden, d_kv, w_kv, d_q, w_q_heads).reshape(batch_dev, seq_dev, depth)

        def ids_of(*values):
            return jnp.concatenate([index(value) for value in values])

        up_c = lax.dynamic_slice_in_dim(w_up, at_c, width_c, axis=1)
        down_c = lax.dynamic_slice_in_dim(w_down, at_c, width_c, axis=0)
        count_a = width_a // block_a
        first_a, block_b, zero = start_a // block_a + core * count_a, start_b // width_b + core, core * 0
        heights = (shared, width_c, width_b, block_a)
        dg_s, dg_c, dg_b, gated = d_gates(ids_of(shared_start // shared + device, zero, block_b, first_a), (w_down, down_c, w_down, w_down), heights, (*heights[:3], width_a), dout_all, 1024)
        gate = (block_a, count_a, start_a // block_a)
        packed, halves, gated = shared_grad(w_down, w_up, dg_s, hidden_all, dout_all, ((keep, recv), (keep_kv, recv_kv)), gated, (shared, shared_start // shared), gate, 1024, 512, inv_div, colour_axes)
        dg_a, up_own, down_own, own_sum = gate_reduce(w_down, up_c, dout_all, dg_c, hidden_all, halves, gated, gate, 1024, 512, inv_div, colour_axes)
        packed_all = lax.all_gather(packed, ('dp', 'cp'), axis=0)
        summed = lax.all_gather(own_sum, ('dp', 'cp'), axis=0)
        splits = (heads // 4, heads // 2)
        dw_q, dw_k, dw_v, dw_o = attn_unpack(summed, unit_of, splits, depth)

        partner = 1 - core
        received_c = (swap(up_own, 'core'), swap(down_own, 'core'))
        part_c = (start_c, width_c)
        *full, up_send, down_send = ffn_grad(ids_of(first_a, start_a + core * width_a, core), w_up, dg_a, hidden_all, dout_all, ffn_width, width_a, block_a, 2048, 1024, inv_div, (part_c, None, 256, 1), (up_own, down_own))
        received_a = (swap(up_send, 'core'), swap(down_send, 'core'))
        *full, up_send, down_send = ffn_grad(ids_of(block_b, start_b + core * width_b, partner), w_up, dg_b, hidden_all, dout_all, ffn_width, width_b, width_b, 1024, 512, inv_div, (part_c, (shared_start, shared), 256, 6), (*received_c, packed_all), full)
        received_b = (swap(up_send, 'core'), swap(down_send, 'core'))
        full = assemble(index(partner), (start_a, width_a), received_a, full)
        dw_up, dw_down = assemble(index(partner), (start_b, width_b), received_b, full)
        return d_x, dw_q.transpose(1, 0, 2), dw_k, dw_v, dw_o.reshape(w_o.shape), dw_up, dw_down

    act_spec = P('dp', 'cp', None)
    return jax.shard_map(device_backward, mesh=mesh, in_specs=(act_spec, act_spec, P(), P(), P(), P(), P(), P()), out_specs=(act_spec, P(), P(), P(), P(), P(), P()), check_vma=False)
```
